8 devices in a mesh: parts: 1 (over z), data: 8 (over y, x, core).
Axes of the slice: x: 2, y: 2, z: 1, core: 2. Of those that a mesh axis runs over, the one named last changes fastest.
Arguments:
- feats: bfloat16 [8192, 784], P('data')
- labels: int32 [8192], P('data')
- w_in: float32 [784, 4, 800], P(None, 'parts')
- w_out: float32 [4, 800], P('parts')
- mom_in: float32 [784, 4, 800], P(None, 'parts')
- mom_out: float32 [4, 800], P('parts')
Outputs:
- output 1: float32 [784, 4, 800], P(None, 'parts')
- output 2: float32 [4, 800], P('parts')
- output 3: float32 [784, 4, 800], P(None, 'parts')
- output 4: float32 [4, 800], P('parts')
- output 5: float32 [4], P('parts')
All inputs are finite; a program needn't handle non-finite values.
Results may differ from the reference program's by a relative error of at most 0.001.
Values are sent between devices in bfloat16 or wider.
A program may use at most 1 GiB of HBM per device.

```python
import math
import jax
import jax.numpy as jnp
from jax import lax

D = 784
HIDDEN = 800
CHAINS = 4
ROWS_DEV = 1024
GROUP = 8
LEAPS = 16
N_ROWS = ROWS_DEV * GROUP
STEP = 1.0 / math.sqrt(N_ROWS * (D + HIDDEN))
PRIOR_VAR = 1.0


def setup_inputs(seed: int = 0, part: int = 0) -> dict:
    key = jax.random.key(seed)
    key_mean, key_noise, key_rate, key_draw, key_part = jax.random.split(key, 5)
    centers = jax.random.normal(key_mean, (GROUP, 1, D), jnp.float32)
    noise = jax.random.normal(key_noise, (GROUP, ROWS_DEV, D), jnp.float32)
    feats = (centers + noise).reshape(N_ROWS, D).astype(jnp.bfloat16)
    rates = jax.random.randint(key_rate, (GROUP, 1), 50, 951)
    draws = jax.random.randint(key_draw, (GROUP, ROWS_DEV), 0, 1000)
    labels = (draws < rates).astype(jnp.int32).reshape(N_ROWS)
    part_key = jax.random.fold_in(key_part, part)
    key_w1, key_w2, key_m1, key_m2 = jax.random.split(part_key, 4)
    w_in = jax.random.normal(key_w1, (D, CHAINS, HIDDEN), jnp.float32) * (2.0 * D) ** -0.5
    w_out = jax.random.normal(key_w2, (CHAINS, HIDDEN), jnp.float32) * (1.5 * HIDDEN ** -0.5)
    mom_in = jax.random.normal(key_m1, (D, CHAINS, HIDDEN), jnp.float32)
    mom_out = jax.random.normal(key_m2, (CHAINS, HIDDEN), jnp.float32)
    return {'feats': feats, 'labels': labels, 'w_in': w_in, 'w_out': w_out, 'mom_in': mom_in, 'mom_out': mom_out}


def block_terms(x_rows, lab_rows, w_flat, w_out):
    pre_act = jnp.dot(x_rows, w_flat, preferred_element_type=jnp.float32).reshape(ROWS_DEV, CHAINS, HIDDEN)
    hidden_act = jnp.tanh(pre_act)
    logits = jnp.sum(hidden_act * w_out, axis=-1)
    residual = lab_rows[:, None] - jax.nn.sigmoid(logits)
    grad_out = jnp.sum(hidden_act * residual[:, :, None], axis=0)
    back_grad = (residual[:, :, None] * w_out * (1.0 - hidden_act * hidden_act)).astype(jnp.bfloat16)
    grad_in = jnp.dot(x_rows.T, back_grad.reshape(ROWS_DEV, CHAINS * HIDDEN), preferred_element_type=jnp.float32)
    return grad_in.reshape(D, CHAINS, HIDDEN), grad_out, logits


def log_post_grad(x_blocks, lab_blocks, w_in, w_out):
    w_flat = w_in.astype(jnp.bfloat16).reshape(D, CHAINS * HIDDEN)

    def row_block(acc_sum, block_in):
        grad_in, grad_out, logits = block_terms(block_in[0], block_in[1], w_flat, w_out)
        return (acc_sum[0] + grad_in, acc_sum[1] + grad_out), logits

    sums, logits = lax.scan(row_block, (jnp.zeros_like(w_in), jnp.zeros_like(w_out)), (x_blocks, lab_blocks))
    return sums[0] - w_in / PRIOR_VAR, sums[1] - w_out / PRIOR_VAR, logits


def reference(feats, labels, w_in, w_out, mom_in, mom_out):
    x_blocks = feats.reshape(GROUP, ROWS_DEV, D)
    lab_blocks = labels.astype(jnp.float32).reshape(GROUP, ROWS_DEV)
    grad_in, grad_out, logits = log_post_grad(x_blocks, lab_blocks, w_in, w_out)
    mom_in = mom_in + 0.5 * STEP * grad_in
    mom_out = mom_out + 0.5 * STEP * grad_out

    def leap_step(state_now, unused):
        pos_in, pos_out, vel_in, vel_out = state_now
        pos_in = pos_in + STEP * vel_in
        pos_out = pos_out + STEP * vel_out
        g_in, g_out, g_logits = log_post_grad(x_blocks, lab_blocks, pos_in, pos_out)
        return (pos_in, pos_out, vel_in + STEP * g_in, vel_out + STEP * g_out), None

    state_end, unused_out = lax.scan(leap_step, (w_in, w_out, mom_in, mom_out), None, length=LEAPS - 1)
    pos_in, pos_out, vel_in, vel_out = state_end
    pos_in = pos_in + STEP * vel_in
    pos_out = pos_out + STEP * vel_out
    grad_in, grad_out, logits = log_post_grad(x_blocks, lab_blocks, pos_in, pos_out)
    vel_in = vel_in + 0.5 * STEP * grad_in
    vel_out = vel_out + 0.5 * STEP * grad_out
    row_loss = jnp.sum(jax.nn.softplus(logits) - lab_blocks[:, :, None] * logits, axis=(0, 1))
    energy = row_loss + (jnp.sum(pos_in * pos_in, axis=(0, 2)) + jnp.sum(pos_out * pos_out, axis=1)) / (2.0 * PRIOR_VAR) + 0.5 * (jnp.sum(vel_in * vel_in, axis=(0, 2)) + jnp.sum(vel_out * vel_out, axis=1))
    return pos_in, pos_out, vel_in, vel_out, energy
```

```python
import functools
import math
import jax
import jax.numpy as jnp
from jax import lax
from jax.experimental import pallas as pl
from jax.experimental.pallas import tpu as pltpu
from jax.sharding import PartitionSpec as P

LEAPS = 16
PRIOR_VAR = 1.0
MAIN = 768
BLOCK = 2048
CHUNK = 512
DEPTH = 512
MESH = pl.DeviceIdType.MESH
F32 = jnp.float32
BF16 = jnp.bfloat16
NT = (((1,), (1,)), ((), ()))


def chain_kernel(step, xm_hbm, xr_hbm, lab_ref, wm0, wr0, v0, pm0, pr0, q0,
                 wm, wr, v, pm, pr, q, energy,
                 xm, xr, act, bt, gm, gr, g2, wmb, wrb, z_own, z_peer,
                 load_sem, send_sem, recv_sem):
    num_rows = xm.shape[0]
    num_block = num_rows // BLOCK
    me = lax.axis_index("data")
    core = lax.rem(me, 2)
    peer = me + 1 - 2 * core

    barrier = pltpu.get_barrier_semaphore()
    pl.semaphore_signal(barrier, inc=1, device_id={"data": peer}, device_id_type=MESH)
    pl.semaphore_wait(barrier, 1)

    load_m = pltpu.make_async_copy(xm_hbm, xm, load_sem.at[0])
    load_r = pltpu.make_async_copy(xr_hbm, xr, load_sem.at[1])
    load_m.start()
    load_r.start()
    wm[...] = wm0[...]
    wr[...] = wr0[...]
    v[...] = v0[...]
    pm[...] = pm0[...]
    pr[...] = pr0[...]
    q[...] = q0[...]
    wmb[...] = wm0[...].astype(BF16)
    wrb[...] = wr0[...].astype(BF16)
    load_m.wait()
    load_r.wait()

    def z_copy(slot, block):
        span = pl.ds(block * BLOCK, BLOCK)
        return pltpu.make_async_remote_copy(
            src_ref=z_own.at[slot, :, span], dst_ref=z_peer.at[slot, :, span],
            send_sem=send_sem.at[slot, block], recv_sem=recv_sem.at[slot, block],
            device_id={"data": peer}, device_id_type=MESH)

    def forward(block, slot):
        base = block * BLOCK
        for n in range(BLOCK // CHUNK):
            rows = pl.ds(pl.multiple_of(base + n * CHUNK, CHUNK), CHUNK)
            pre = lax.dot_general(wmb[...], xm[rows, :], NT, preferred_element_type=F32)
            pre = pre + jnp.dot(wrb[...], xr[:, rows], preferred_element_type=F32)
            for j in range(CHUNK // 128):
                cols = pl.ds(pl.multiple_of(base + n * CHUNK + j * 128, 128), 128)
                t = jnp.tanh(pre[:, j * 128:(j + 1) * 128])
                act[:, cols] = t
                z_own[slot, :, cols] = jnp.sum(t * v[...], axis=0, keepdims=True)
        z_copy(slot, block).start()

    def backward(block, slot):
        z_copy(slot, block).wait()
        base = block * BLOCK
        for n in range(BLOCK // DEPTH):
            for j in range(DEPTH // 128):
                cols = pl.ds(pl.multiple_of(base + n * DEPTH + j * 128, 128), 128)
                z = z_own[slot, :, cols] + z_peer[slot, :, cols]
                r = lab_ref[:, cols] - jax.nn.sigmoid(z)
                t = act[:, cols]
                rb = jnp.broadcast_to(r, t.shape)
                bt[:, pl.ds(n * DEPTH + j * 128, 128)] = ((rb * v[...]) * (1.0 - t * t)).astype(BF16)
                g2[...] += rb * t
            rows = pl.ds(pl.multiple_of(base + n * DEPTH, DEPTH), DEPTH)
            b = bt[:, n * DEPTH:(n + 1) * DEPTH]
            gm[...] += jnp.dot(b, xm[rows, :], preferred_element_type=F32)
            gr[...] += lax.dot_general(b, xr[:, rows], NT, preferred_element_type=F32)

    def gradient(index, carry):
        slot = lax.rem(index, 2)
        edge = jnp.logical_or(index == 0, index == LEAPS)
        kick = jnp.where(edge, 0.5 * step, step).astype(F32)
        drift = jnp.where(index == LEAPS, 0.0, step).astype(F32)
        gm[...] = jnp.zeros_like(gm)
        gr[...] = jnp.zeros_like(gr)
        g2[...] = jnp.zeros_like(g2)

        def fwd(block, c):
            forward(block, slot)
            return c

        def bwd(block, c):
            backward(block, slot)
            return c

        lax.fori_loop(0, num_block, fwd, 0)
        lax.fori_loop(0, num_block, bwd, 0)

        def update(w, p, g, wb):
            new_p = p[...] + kick * (g - w[...] / PRIOR_VAR)
            p[...] = new_p
            new_w = w[...] + drift * new_p
            w[...] = new_w
            if wb is not None:
                wb[...] = new_w.astype(BF16)

        update(wm, pm, gm[...], wmb)
        update(wr, pr, gr[...], wrb)
        update(v, q, jnp.broadcast_to(jnp.sum(g2[...], axis=1, keepdims=True), g2.shape), None)
        return carry

    lax.fori_loop(0, LEAPS + 1, gradient, 0)
    last = LEAPS % 2
    z = z_own[last] + z_peer[last]
    loss = jnp.maximum(z, 0.0) + jnp.log1p(jnp.exp(-jnp.abs(z))) - lab_ref[...] * z

    def total(x):
        return jnp.sum(jnp.sum(x, axis=0, keepdims=True), axis=1, keepdims=True)

    squares = total(wm[...] * wm[...]) + total(wr[...] * wr[...]) + total(v[...] * v[...]) / 128.0
    moving = total(pm[...] * pm[...]) + total(pr[...] * pr[...]) + total(q[...] * q[...]) / 128.0
    mine = 0.5 * total(loss) + squares / (2.0 * PRIOR_VAR) + 0.5 * moving
    energy[...] = jnp.broadcast_to(mine, energy.shape)


def run_kernel(step, xm, xr, lab, state):
    num_rows = xm.shape[0]
    half = state[0].shape[0]
    vmem = pl.BlockSpec(memory_space=pltpu.VMEM)
    hbm = pl.BlockSpec(memory_space=pl.ANY)
    rest = xr.shape[0]
    shapes = [jax.ShapeDtypeStruct(s.shape, F32) for s in state] + [jax.ShapeDtypeStruct((1, 128), F32)]
    return pl.pallas_call(
        functools.partial(chain_kernel, step),
        out_shape=shapes,
        in_specs=[hbm, hbm] + [vmem] * 7,
        out_specs=[vmem] * 7,
        scratch_shapes=[
            pltpu.VMEM((num_rows, MAIN), BF16),
            pltpu.VMEM((rest, num_rows), BF16),
            pltpu.VMEM((half, num_rows), F32),
            pltpu.VMEM((half, BLOCK), BF16),
            pltpu.VMEM((half, MAIN), F32),
            pltpu.VMEM((half, rest), F32),
            pltpu.VMEM((half, 128), F32),
            pltpu.VMEM((half, MAIN), BF16),
            pltpu.VMEM((half, rest), BF16),
            pltpu.VMEM((2, 1, num_rows), F32),
            pltpu.VMEM((2, 1, num_rows), F32),
            pltpu.SemaphoreType.DMA((2,)),
            pltpu.SemaphoreType.DMA((2, num_rows // BLOCK)),
            pltpu.SemaphoreType.DMA((2, num_rows // BLOCK)),
        ],
        compiler_params=pltpu.CompilerParams(
            collective_id=0, has_side_effects=True, vmem_limit_bytes=60 * 2 ** 20),
    )(xm, xr, lab, *state)


def solution(mesh):
    row_spec = P('data', None)
    label_spec = P('data')
    in_spec = P(None, 'parts', None)
    out_spec = P('parts', None)
    chain_spec = P('parts')

    def run_chains(feats, labels, w_in, w_out, mom_in, mom_out):
        num_rows, num_feat = feats.shape
        hidden = w_in.shape[2]
        chains = w_in.shape[1]
        half = hidden // 2
        step = 1.0 / math.sqrt(num_rows * (num_feat + hidden))

        def device_body(x_rows, y_rows, w1, w2, p1, p2):
            me = lax.axis_index('data')
            chain, core = me // 2, me % 2
            xm = lax.all_gather(x_rows[:, :MAIN], 'data', axis=0, tiled=True)
            xr = lax.all_gather(x_rows[:, MAIN:].T, 'data', axis=0)
            xr = jnp.moveaxis(xr, 0, 1).reshape(num_feat - MAIN, num_rows)
            lab = lax.all_gather(y_rows, 'data', axis=0, tiled=True).astype(F32)[None, :]

            def mine_in(w):
                w = lax.dynamic_slice(w, (0, chain, core * half), (num_feat, 1, half))[:, 0, :].T
                return w[:, :MAIN], w[:, MAIN:]

            def mine_out(u):
                u = lax.dynamic_slice(u, (chain, core * half), (1, half))
                return jnp.broadcast_to(u.T, (half, 128))

            state = (*mine_in(w1), mine_out(w2), *mine_in(p1), mine_out(p2))
            wm, wr, v, pm, pr, q, energy = run_kernel(step, xm, xr, lab, state)

            def all_in(m, r):
                mine = jnp.concatenate([m, r], axis=1).T
                every = lax.all_gather(mine, 'data', axis=0)
                every = every.reshape(chains, 2, num_feat, half)
                return jnp.transpose(every, (2, 0, 1, 3)).reshape(num_feat, chains, hidden)

            def all_out(u):
                return lax.all_gather(u[:, 0], 'data', axis=0).reshape(chains, hidden)

            total = lax.all_gather(energy[0, :1], 'data', axis=0).reshape(chains, 2).sum(axis=1)
            return all_in(wm, wr), all_out(v), all_in(pm, pr), all_out(q), total

        mapped = jax.shard_map(device_body, mesh=mesh, in_specs=(row_spec, label_spec, in_spec, out_spec, in_spec, out_spec), out_specs=(in_spec, out_spec, in_spec, out_spec, chain_spec), check_vma=False)
        return mapped(feats, labels, w_in, w_out, mom_in, mom_out)

    return run_chains
```

```python
import functools
import math
import jax
import jax.numpy as jnp
from jax import lax
from jax.experimental import pallas as pl
from jax.experimental.pallas import tpu as pltpu
from jax.sharding import PartitionSpec as P

LEAPS = 16
PRIOR_VAR = 1.0
MAIN = 768
BLOCK = 2048
CHUNK = 512
DEPTH = 512
PIECE = 512
SMALL = 24
MESH = pl.DeviceIdType.MESH
F32 = jnp.float32
BF16 = jnp.bfloat16
NT = (((1,), (1,)), ((), ()))


def chain_kernel(step, x_hbm, xr_ref, lab_ref, w1_hbm, w2_ref, p1_hbm, p2_ref,
                 end_w, end_ws, end_p, end_ps,
                 xm, xr, lab, stage, turn, act, bt, gm, gr, g2, wm, wr, v, pm, pr, q, wmb, wrb,
                 z_own, z_peer, small_w, small_p,
                 load_sem, x_send, x_recv, send_sem, recv_sem, end_send, end_recv, end_load):
    num_rows = xm.shape[0]
    num_block = num_rows // BLOCK
    half = wm.shape[0]
    rest = xr.shape[0]
    me = lax.axis_index("data")
    chip = me // 2
    core = lax.rem(me, 2)
    x_bit = lax.rem(chip, 2)
    y_bit = chip // 2
    peer = me + 1 - 2 * core
    x_near = me + 2 - 4 * x_bit
    y_near = me + 4 - 8 * y_bit
    far = x_near + 4 - 8 * y_bit

    barrier = pltpu.get_barrier_semaphore()
    for other in (peer, x_near, y_near):
        pl.semaphore_signal(barrier, inc=1, device_id={"data": other}, device_id_type=MESH)

    def rows_of(position, size):
        return pl.ds(pl.multiple_of(position * size, size), size)

    own = [2 * core, 2 * core + 1]
    mine = rows_of(core, 2 * PIECE)
    loads = [
        pltpu.make_async_copy(x_hbm.at[:, pl.ds(0, MAIN)], xm.at[mine, :], load_sem.at[0]),
        pltpu.make_async_copy(xr_ref, xr.at[:, mine], load_sem.at[1]),
        pltpu.make_async_copy(lab_ref, lab.at[:, mine], load_sem.at[2]),
    ]
    for c in loads:
        c.start()
    load_w = pltpu.make_async_copy(w1_hbm, stage, load_sem.at[3])
    load_p = pltpu.make_async_copy(p1_hbm, stage, load_sem.at[4])
    load_w.start()
    pl.semaphore_wait(barrier, 3)
    for c in loads:
        c.wait()

    def x_copies(src, dst, device, ticket):
        a, b = rows_of(src, PIECE), rows_of(dst, PIECE)
        pairs = ((xm.at[a, :], xm.at[b, :]), (xr.at[:, a], xr.at[:, b]), (lab.at[:, a], lab.at[:, b]))
        return [pltpu.make_async_remote_copy(
            src_ref=s, dst_ref=d, send_sem=x_send.at[i, ticket], recv_sem=x_recv.at[i, dst],
            device_id={"data": device}, device_id_type=MESH) for i, (s, d) in enumerate(pairs)]

    def x_go(src, dst, device, ticket):
        for c in x_copies(src, dst, device, ticket):
            c.start()

    def x_arrived(position):
        for c in x_copies(position, position, peer, 0):
            c.wait_recv()

    def x_sent(ticket):
        for c in x_copies(0, 0, peer, ticket):
            c.wait_send()

    def near_pos(h, which, owner):
        return 4 + 4 * h + 2 * which + owner

    def far_pos(h, owner):
        return 12 + 2 * h + owner

    for h in range(2):
        x_go(own[h], near_pos(h, 0, core), x_near, 3 * h)
        x_go(own[h], near_pos(h, 1, core), y_near, 3 * h + 1)
        x_go(own[h], own[h], peer, 3 * h + 2)

    def part_of(w, m, r, as_bf16):
        for d in range(MAIN // 128):
            turn[:, d * 128:(d + 1) * 128] = stage[d * 128:(d + 1) * 128, chip, :].T
        span = pl.ds(pl.multiple_of(core * half, 8), half)
        m[...] = turn[span, :]
        tail = stage[MAIN:MAIN + rest, chip, :]
        tail = jnp.concatenate([tail, jnp.zeros((128 - rest, tail.shape[1]), F32)], axis=0)
        turn[:, 0:128] = tail.T
        r[...] = turn[span, 0:rest]

    def row_of(u, out):
        turn[:, 0:128] = jnp.broadcast_to(u[pl.ds(chip, 1), :], (128, u.shape[1])).T
        out[...] = turn[pl.ds(pl.multiple_of(core * half, 8), half), 0:128]

    load_w.wait()
    part_of(None, wm, wr, True)
    load_p.start()
    row_of(w2_ref, v)
    wmb[...] = wm[...].astype(BF16)
    wrb[...] = wr[...].astype(BF16)
    row_of(p2_ref, q)
    load_p.wait()
    part_of(None, pm, pr, False)

    other = 1 - core
    x_arrived(2 * other)
    x_arrived(2 * other + 1)

    def arrivals(k):
        if k == 1:
            for which in range(2):
                x_arrived(near_pos(0, which, core))
                if which == 0:
                    x_go(near_pos(0, 0, core), far_pos(0, core), y_near, 6)
                x_go(near_pos(0, which, core), near_pos(0, which, core), peer, 7 + which)
            for which in range(2):
                x_arrived(near_pos(0, which, other))
        elif k == 2:
            for which in (1, 0):
                x_arrived(near_pos(1, which, core))
                if which == 1:
                    x_go(near_pos(1, 1, core), far_pos(1, core), x_near, 9)
                x_go(near_pos(1, which, core), near_pos(1, which, core), peer, 10 + which)
            for which in range(2):
                x_arrived(near_pos(1, which, other))
        elif k == 3:
            for h in range(2):
                x_arrived(far_pos(h, core))
                x_go(far_pos(h, core), far_pos(h, core), peer, 12 + h)
            for h in range(2):
                x_arrived(far_pos(h, other))

    def z_copy(slot, block):
        span = rows_of(block, BLOCK)
        return pltpu.make_async_remote_copy(
            src_ref=z_own.at[slot, :, span], dst_ref=z_peer.at[slot, :, span],
            send_sem=send_sem.at[slot, block], recv_sem=recv_sem.at[slot, block],
            device_id={"data": peer}, device_id_type=MESH)

    def forward(block, slot):
        base = block * BLOCK
        for n in range(BLOCK // CHUNK):
            rows = pl.ds(pl.multiple_of(base + n * CHUNK, CHUNK), CHUNK)
            pre = lax.dot_general(wmb[...], xm[rows, :], NT, preferred_element_type=F32)
            pre = pre + jnp.dot(wrb[...], xr[:, rows], preferred_element_type=F32)
            for j in range(CHUNK // 128):
                cols = pl.ds(pl.multiple_of(base + n * CHUNK + j * 128, 128), 128)
                t = jnp.tanh(pre[:, j * 128:(j + 1) * 128])
                act[:, cols] = t
                z_own[slot, :, cols] = jnp.sum(t * v[...], axis=0, keepdims=True)
        z_copy(slot, block).start()

    def backward(block, slot):
        z_copy(slot, block).wait()
        base = block * BLOCK
        for n in range(BLOCK // DEPTH):
            for j in range(DEPTH // 128):
                cols = pl.ds(pl.multiple_of(base + n * DEPTH + j * 128, 128), 128)
                z = z_own[slot, :, cols] + z_peer[slot, :, cols]
                r = lab[:, cols] - jax.nn.sigmoid(z)
                t = act[:, cols]
                rb = jnp.broadcast_to(r, t.shape)
                bt[:, pl.ds(n * DEPTH + j * 128, 128)] = ((rb * v[...]) * (1.0 - t * t)).astype(BF16)
                g2[...] += rb * t
            rows = pl.ds(pl.multiple_of(base + n * DEPTH, DEPTH), DEPTH)
            b = bt[:, n * DEPTH:(n + 1) * DEPTH]
            gm[...] += jnp.dot(b, xm[rows, :], preferred_element_type=F32)
            gr[...] += lax.dot_general(b, xr[:, rows], NT, preferred_element_type=F32)

    big = (wm, pm)
    small = (small_w, small_p)
    out_big = (end_w, end_p)
    out_small = (end_ws, end_ps)
    part = half // 2

    def end_pair(t, piece, source):
        if piece == 2:
            return small[t], out_small[t].at[source]
        span = pl.ds(piece * part, part)
        return big[t].at[span, :], out_big[t].at[source, span, :]

    def end_copy(t, piece, source, device, ticket, first):
        src, dst = end_pair(t, piece, source)
        return pltpu.make_async_remote_copy(
            src_ref=src if first else dst, dst_ref=dst,
            send_sem=end_send.at[t, piece, ticket], recv_sem=end_recv.at[t, piece, source],
            device_id={"data": device}, device_id_type=MESH)

    def end_arrived(t, piece, source):
        end_copy(t, piece, source, peer, 0, False).wait_recv()

    def end_begin(t):
        for piece in (0, 2, 1):
            end_copy(t, piece, me, x_near, 0, True).start()
            end_copy(t, piece, me, y_near, 1, True).start()
        for piece in (0, 1, 2):
            end_copy(t, piece, me, peer, 2, True).start()
            src, dst = end_pair(t, piece, me)
            pltpu.make_async_copy(src, dst, end_load.at[t, piece]).start()

    def end_relay(t):
        for piece in (0, 2, 1):
            end_arrived(t, piece, x_near)
            if piece != 1:
                end_copy(t, piece, x_near, y_near, 3, False).start()
            end_arrived(t, piece, y_near)
            if piece == 1:
                end_copy(t, piece, y_near, x_near, 3, False).start()
            end_copy(t, piece, x_near, peer, 4, False).start()
            end_copy(t, piece, y_near, peer, 5, False).start()

    def end_finish(t):
        for piece in (0, 2, 1):
            end_arrived(t, piece, far)
            end_copy(t, piece, far, peer, 6, False).start()
        for piece in (0, 1, 2):
            for delta in (me, x_near, y_near, far):
                end_arrived(t, piece, delta + 1 - 2 * core)
            for ticket in range(7):
                end_copy(t, piece, me, peer, ticket, False).wait_send()
            src, dst = end_pair(t, piece, me)
            pltpu.make_async_copy(src, dst, end_load.at[t, piece]).wait()

    def pack_small(buf, r, u, extra):
        wide = jnp.concatenate([r[...], u[:, 0:8], jnp.zeros((half, 104), F32)], axis=1)
        flat = wide.T
        buf[0:rest, :] = flat[0:rest, :]
        buf[rest:SMALL, :] = jnp.where(lax.broadcasted_iota(jnp.int32, (SMALL - rest, half), 0) == 0, flat[rest:SMALL, :], extra)

    def gradient(index, carry):
        slot = lax.rem(index, 2)
        edge = jnp.logical_or(index == 0, index == LEAPS)
        kick = jnp.where(edge, 0.5 * step, step).astype(F32)
        gm[...] = jnp.zeros_like(gm)
        gr[...] = jnp.zeros_like(gr)
        g2[...] = jnp.zeros_like(g2)

        def stage_of(k, c):
            for j in range(1, num_block):
                @pl.when(jnp.logical_and(index == 0, k == j))
                def _():
                    arrivals(j)

            @pl.when(k < num_block)
            def _():
                forward(k, slot)

            @pl.when(k > 0)
            def _():
                backward(k - 1, slot)
            return c

        lax.fori_loop(0, num_block + 1, stage_of, 0)

        pm[...] += kick * (gm[...] - wm[...] / PRIOR_VAR)
        pr[...] += kick * (gr[...] - wr[...] / PRIOR_VAR)
        q[...] += kick * (jnp.broadcast_to(jnp.sum(g2[...], axis=1, keepdims=True), g2.shape) - v[...] / PRIOR_VAR)

        @pl.when(index < LEAPS)
        def _():
            new = wm[...] + step * pm[...]
            wm[...] = new
            wmb[...] = new.astype(BF16)
            new = wr[...] + step * pr[...]
            wr[...] = new
            wrb[...] = new.astype(BF16)
            v[...] += step * q[...]

        @pl.when(index == LEAPS - 1)
        def _():
            pack_small(small_w, wr, v, 0.0)
            end_begin(0)
        return carry

    lax.fori_loop(0, LEAPS + 1, gradient, 0)

    last = LEAPS % 2
    z = z_own[last] + z_peer[last]
    loss = jnp.maximum(z, 0.0) + jnp.log1p(jnp.exp(-jnp.abs(z))) - lab[...] * z

    def total(x):
        return jnp.sum(jnp.sum(x, axis=0, keepdims=True), axis=1, keepdims=True)

    squares = total(wm[...] * wm[...]) + total(wr[...] * wr[...]) + total(v[...] * v[...]) / 128.0
    moving = total(pm[...] * pm[...]) + total(pr[...] * pr[...]) + total(q[...] * q[...]) / 128.0
    energy = 0.5 * total(loss) + squares / (2.0 * PRIOR_VAR) + 0.5 * moving
    pack_small(small_p, pr, q, energy)
    end_begin(1)
    end_relay(0)
    end_relay(1)
    end_finish(0)
    end_finish(1)
    for ticket in range(14):
        x_sent(ticket)


def run_kernel(step, xs, xr, lab, w1, w2, p1, p2, devices):
    num_feat, chains, hidden = w1.shape
    num_rows = xs.shape[0] * devices
    half = hidden // 2
    rest = num_feat - MAIN
    vmem = pl.BlockSpec(memory_space=pltpu.VMEM)
    hbm = pl.BlockSpec(memory_space=pl.ANY)
    big = jax.ShapeDtypeStruct((devices, half, MAIN), F32)
    small = jax.ShapeDtypeStruct((devices, SMALL, half), F32)
    blocks = num_rows // BLOCK
    dma = pltpu.SemaphoreType.DMA
    return pl.pallas_call(
        functools.partial(chain_kernel, step),
        out_shape=[big, small, big, small],
        in_specs=[hbm, hbm, hbm, hbm, vmem, hbm, vmem],
        out_specs=[hbm] * 4,
        scratch_shapes=[
            pltpu.VMEM((num_rows, MAIN), BF16),
            pltpu.VMEM((rest, num_rows), BF16),
            pltpu.VMEM((1, num_rows), F32),
            pltpu.VMEM((num_feat, chains, hidden), F32),
            pltpu.VMEM((hidden, MAIN), F32),
            pltpu.VMEM((half, num_rows), F32),
            pltpu.VMEM((half, BLOCK), BF16),
            pltpu.VMEM((half, MAIN), F32),
            pltpu.VMEM((half, rest), F32),
            pltpu.VMEM((half, 128), F32),
            pltpu.VMEM((half, MAIN), F32),
            pltpu.VMEM((half, rest), F32),
            pltpu.VMEM((half, 128), F32),
            pltpu.VMEM((half, MAIN), F32),
            pltpu.VMEM((half, rest), F32),
            pltpu.VMEM((half, 128), F32),
            pltpu.VMEM((half, MAIN), BF16),
            pltpu.VMEM((half, rest), BF16),
            pltpu.VMEM((2, 1, num_rows), F32),
            pltpu.VMEM((2, 1, num_rows), F32),
            pltpu.VMEM((SMALL, half), F32),
            pltpu.VMEM((SMALL, half), F32),
            dma((5,)),
            dma((3, 14)),
            dma((3, 16)),
            dma((2, blocks)),
            dma((2, blocks)),
            dma((2, 3, 7)),
            dma((2, 3, devices)),
            dma((2, 3)),
        ],
        compiler_params=pltpu.CompilerParams(
            collective_id=0, has_side_effects=True, vmem_limit_bytes=62 * 2 ** 20),
    )(xs, xr, lab, w1, w2, p1, p2)


def place_kernel(gw, gws, gp, gps, end_w, end_p):
    step = pl.program_id(0)
    tiles = MAIN // 128
    chains = end_w.shape[1]
    rest = gws.shape[1] - 8

    @pl.when(step < tiles)
    def _():
        for g, end in ((gw, end_w), (gp, end_p)):
            for c in range(chains):
                end[:, c, :] = jnp.concatenate([g[2 * c], g[2 * c + 1]], axis=0).T

    @pl.when(step == tiles)
    def _():
        for g, end in ((gws, end_w), (gps, end_p)):
            for c in range(chains):
                end[0:rest, c, :] = jnp.concatenate([g[2 * c, 0:rest, :], g[2 * c + 1, 0:rest, :]], axis=1)


def place(gw, gws, gp, gps, num_feat, chains, hidden):
    tiles = MAIN // 128
    devices, half = gw.shape[0], gw.shape[1]
    big = pl.BlockSpec((devices, half, 128), lambda i: (0, 0, jnp.minimum(i, tiles - 1)))
    small = pl.BlockSpec(gws.shape, lambda i: (0, 0, 0))
    out = pl.BlockSpec((128, chains, hidden), lambda i: (i, 0, 0))
    shape = jax.ShapeDtypeStruct((num_feat, chains, hidden), F32)
    return pl.pallas_call(
        place_kernel, grid=(tiles + 1,), out_shape=[shape, shape],
        in_specs=[big, small, big, small], out_specs=[out, out],
        compiler_params=pltpu.CompilerParams(vmem_limit_bytes=48 * 2 ** 20),
    )(gw, gws, gp, gps)


def solution(mesh):
    row_spec = P('data', None)
    label_spec = P('data')
    in_spec = P(None, 'parts', None)
    out_spec = P('parts', None)
    chain_spec = P('parts')
    devices = mesh.shape['data']

    def run_chains(feats, labels, w_in, w_out, mom_in, mom_out):
        num_rows, num_feat = feats.shape
        chains, hidden = w_out.shape
        step = 1.0 / math.sqrt(num_rows * (num_feat + hidden))

        def device_body(x_rows, y_rows, w1, w2, p1, p2):
            xr = x_rows[:, MAIN:].T
            lab = y_rows.astype(F32)[None, :]
            gw, gws, gp, gps = run_kernel(step, x_rows, xr, lab, w1, w2, p1, p2, devices)
            end_w, end_p = place(gw, gws, gp, gps, num_feat, chains, hidden)
            rest = num_feat - MAIN
            end_w2 = gws[:, rest, :].reshape(chains, hidden)
            end_p2 = gps[:, rest, :].reshape(chains, hidden)
            energy = gps[:, rest + 1, 0].reshape(chains, 2).sum(axis=1)
            return end_w, end_w2, end_p, end_p2, energy

        mapped = jax.shard_map(device_body, mesh=mesh, in_specs=(row_spec, label_spec, in_spec, out_spec, in_spec, out_spec), out_specs=(in_spec, out_spec, in_spec, out_spec, chain_spec), check_vma=False)
        return mapped(feats, labels, w_in, w_out, mom_in, mom_out)

    return run_chains
```

```python
import functools
import math
import jax
import jax.numpy as jnp
from jax import lax
from jax.experimental import pallas as pl
from jax.experimental.pallas import tpu as pltpu
from jax.sharding import PartitionSpec as P

LEAPS = 16
PRIOR_VAR = 1.0
MAIN = 768
BLOCK = 4096
CHUNK = 256
DEPTH = 512
PIECE = 512
SMALL = 24
MESH = pl.DeviceIdType.MESH
F32 = jnp.float32
BF16 = jnp.bfloat16
NT = (((1,), (1,)), ((), ()))


def chain_kernel(step, x_hbm, lab_ref, w1_hbm, w2_ref, p1_hbm, p2_ref,
                 end_w, end_ws, end_p, end_ps,
                 xt, lab, stage, turn, act, bt, gm, g2, wm, v, pm, q, wmb,
                 z_own, z_peer, small_w, small_p,
                 load_sem, x_send, x_recv, send_sem, recv_sem, end_send, end_recv, end_load):
    num_feat, num_rows = xt.shape
    num_block = num_rows // BLOCK
    half = wm.shape[0]
    rest = num_feat - MAIN
    me = lax.axis_index("data")
    chip = me // 2
    core = lax.rem(me, 2)
    x_bit = lax.rem(chip, 2)
    y_bit = chip // 2
    peer = me + 1 - 2 * core
    x_near = me + 2 - 4 * x_bit
    y_near = me + 4 - 8 * y_bit
    far = x_near + 4 - 8 * y_bit

    barrier = pltpu.get_barrier_semaphore()
    for other in (peer, x_near, y_near):
        pl.semaphore_signal(barrier, inc=1, device_id={"data": other}, device_id_type=MESH)

    def rows_of(position, size):
        return pl.ds(pl.multiple_of(position * size, size), size)

    own = [2 * core, 2 * core + 1]
    mine = rows_of(core, 2 * PIECE)
    loads = [
        pltpu.make_async_copy(x_hbm, xt.at[:, mine], load_sem.at[0]),
        pltpu.make_async_copy(lab_ref, lab.at[:, mine], load_sem.at[1]),
    ]
    for c in loads:
        c.start()
    load_w = pltpu.make_async_copy(w1_hbm, stage, load_sem.at[2])
    load_p = pltpu.make_async_copy(p1_hbm, stage, load_sem.at[3])
    load_w.start()
    pl.semaphore_wait(barrier, 3)
    for c in loads:
        c.wait()

    def x_copies(src, dst, device, ticket):
        a, b = rows_of(src, PIECE), rows_of(dst, PIECE)
        pairs = ((xt.at[:, a], xt.at[:, b]), (lab.at[:, a], lab.at[:, b]))
        return [pltpu.make_async_remote_copy(
            src_ref=s, dst_ref=d, send_sem=x_send.at[i, ticket], recv_sem=x_recv.at[i, dst],
            device_id={"data": device}, device_id_type=MESH) for i, (s, d) in enumerate(pairs)]

    def x_go(src, dst, device, ticket):
        for c in x_copies(src, dst, device, ticket):
            c.start()

    def x_arrived(position):
        for c in x_copies(position, position, peer, 0):
            c.wait_recv()

    def x_sent(ticket):
        for c in x_copies(0, 0, peer, ticket):
            c.wait_send()

    def near_pos(h, which, owner):
        return 4 + 4 * h + 2 * which + owner

    def far_pos(h, owner):
        return 12 + 2 * h + owner

    for h in range(2):
        x_go(own[h], near_pos(h, 0, core), x_near, 3 * h)
        x_go(own[h], near_pos(h, 1, core), y_near, 3 * h + 1)
        x_go(own[h], own[h], peer, 3 * h + 2)

    def part_of(out):
        for d in range(MAIN // 128):
            turn[:, d * 128:(d + 1) * 128] = stage[d * 128:(d + 1) * 128, chip, :].T
        tail = stage[MAIN:MAIN + rest, chip, :]
        tail = jnp.concatenate([tail, jnp.zeros((128 - rest, tail.shape[1]), F32)], axis=0)
        turn[:, MAIN:MAIN + rest] = tail.T[:, 0:rest]
        out[...] = turn[pl.ds(pl.multiple_of(core * half, 8), half), :]

    def row_of(u, out):
        turn[:, 0:128] = jnp.broadcast_to(u[pl.ds(chip, 1), :], (128, u.shape[1])).T
        out[...] = turn[pl.ds(pl.multiple_of(core * half, 8), half), 0:128]

    load_w.wait()
    part_of(wm)
    load_p.start()
    row_of(w2_ref, v)
    wmb[...] = wm[...].astype(BF16)
    row_of(p2_ref, q)
    load_p.wait()
    part_of(pm)
    gm[...] = jnp.zeros_like(gm)
    g2[...] = jnp.zeros_like(g2)

    other = 1 - core
    x_arrived(2 * other)
    x_arrived(2 * other + 1)

    def arrivals(k):
        if k == 1:
            for which in range(2):
                x_arrived(near_pos(0, which, core))
                if which == 0:
                    x_go(near_pos(0, 0, core), far_pos(0, core), y_near, 6)
                x_go(near_pos(0, which, core), near_pos(0, which, core), peer, 7 + which)
            for which in range(2):
                x_arrived(near_pos(0, which, other))
        elif k == 2:
            for which in (1, 0):
                x_arrived(near_pos(1, which, core))
                if which == 1:
                    x_go(near_pos(1, 1, core), far_pos(1, core), x_near, 9)
                x_go(near_pos(1, which, core), near_pos(1, which, core), peer, 10 + which)
            for which in range(2):
                x_arrived(near_pos(1, which, other))
        elif k == 3:
            for h in range(2):
                x_arrived(far_pos(h, core))
                x_go(far_pos(h, core), far_pos(h, core), peer, 12 + h)
            for h in range(2):
                x_arrived(far_pos(h, other))

    def z_copy(slot, block):
        span = rows_of(block, BLOCK)
        return pltpu.make_async_remote_copy(
            src_ref=z_own.at[slot, :, span], dst_ref=z_peer.at[slot, :, span],
            send_sem=send_sem.at[slot, block], recv_sem=recv_sem.at[slot, block],
            device_id={"data": peer}, device_id_type=MESH)

    def forward(block, slot):
        base = block * BLOCK
        for n in range(BLOCK // CHUNK):
            rows = pl.ds(pl.multiple_of(base + n * CHUNK, CHUNK), CHUNK)
            pre = jnp.dot(wmb[:, 0:MAIN], xt[0:MAIN, rows], preferred_element_type=F32)
            pre = pre + jnp.dot(wmb[:, MAIN:], xt[MAIN:, rows], preferred_element_type=F32)
            for j in range(CHUNK // 128):
                cols = pl.ds(pl.multiple_of(base + n * CHUNK + j * 128, 128), 128)
                t = jnp.tanh(pre[:, j * 128:(j + 1) * 128])
                act[:, cols] = t
                z_own[slot, :, cols] = jnp.sum(t * v[...], axis=0, keepdims=True)
        z_copy(slot, block).start()

    def backward(block, slot):
        z_copy(slot, block).wait()
        base = block * BLOCK
        for n in range(BLOCK // DEPTH):
            for j in range(DEPTH // 128):
                cols = pl.ds(pl.multiple_of(base + n * DEPTH + j * 128, 128), 128)
                z = z_own[slot, :, cols] + z_peer[slot, :, cols]
                r = lab[:, cols].astype(F32) - jax.nn.sigmoid(z)
                t = act[:, cols]
                rb = jnp.broadcast_to(r, t.shape)
                bt[:, pl.ds(n * DEPTH + j * 128, 128)] = ((rb * v[...]) * (1.0 - t * t)).astype(BF16)
                g2[...] += rb * t
            rows = pl.ds(pl.multiple_of(base + n * DEPTH, DEPTH), DEPTH)
            b = bt[:, n * DEPTH:(n + 1) * DEPTH]
            gm[...] += lax.dot_general(b, xt[:, rows], NT, preferred_element_type=F32)

    big = (wm, pm)
    small = (small_w, small_p)
    out_big = (end_w, end_p)
    out_small = (end_ws, end_ps)
    part = half // 2

    def end_pair(t, piece, source):
        if piece == 2:
            return small[t], out_small[t].at[source]
        span = pl.ds(piece * part, part)
        return big[t].at[span, pl.ds(0, MAIN)], out_big[t].at[source, span, :]

    def end_copy(t, piece, source, device, ticket, first):
        src, dst = end_pair(t, piece, source)
        return pltpu.make_async_remote_copy(
            src_ref=src if first else dst, dst_ref=dst,
            send_sem=end_send.at[t, piece, ticket], recv_sem=end_recv.at[t, piece, source],
            device_id={"data": device}, device_id_type=MESH)

    def end_arrived(t, piece, source):
        end_copy(t, piece, source, peer, 0, False).wait_recv()

    def end_begin(t):
        for piece in (0, 2, 1):
            end_copy(t, piece, me, x_near, 0, True).start()
            end_copy(t, piece, me, y_near, 1, True).start()
        for piece in (0, 1, 2):
            end_copy(t, piece, me, peer, 2, True).start()
            src, dst = end_pair(t, piece, me)
            pltpu.make_async_copy(src, dst, end_load.at[t, piece]).start()

    def end_relay(t):
        for piece in (0, 2, 1):
            end_arrived(t, piece, x_near)
            if piece != 1:
                end_copy(t, piece, x_near, y_near, 3, False).start()
            end_arrived(t, piece, y_near)
            if piece == 1:
                end_copy(t, piece, y_near, x_near, 3, False).start()
            end_copy(t, piece, x_near, peer, 4, False).start()
            end_copy(t, piece, y_near, peer, 5, False).start()

    def end_finish(t):
        for piece in (0, 2, 1):
            end_arrived(t, piece, far)
            end_copy(t, piece, far, peer, 6, False).start()
        for piece in (0, 1, 2):
            for delta in (me, x_near, y_near, far):
                end_arrived(t, piece, delta + 1 - 2 * core)
            for ticket in range(7):
                end_copy(t, piece, me, peer, ticket, False).wait_send()
            src, dst = end_pair(t, piece, me)
            pltpu.make_async_copy(src, dst, end_load.at[t, piece]).wait()

    def pack_small(buf, m, u, extra):
        wide = jnp.concatenate([m[:, MAIN:MAIN + rest], u[:, 0:8], jnp.zeros((half, 104), F32)], axis=1)
        flat = wide.T
        buf[0:rest, :] = flat[0:rest, :]
        buf[rest:SMALL, :] = jnp.where(lax.broadcasted_iota(jnp.int32, (SMALL - rest, half), 0) == 0, flat[rest:SMALL, :], extra)

    def gradient(index, carry):
        slot = lax.rem(index, 2)
        edge = jnp.logical_or(index == 0, index == LEAPS)
        kick = jnp.where(edge, 0.5 * step, step).astype(F32)
        def stage_of(k, c):
            for j in range(1, 4):
                @pl.when(jnp.logical_and(index == 0, k == j * 4 * PIECE // BLOCK))
                def _():
                    arrivals(j)

            @pl.when(k < num_block)
            def _():
                forward(k, slot)

            @pl.when(k > 0)
            def _():
                backward(k - 1, slot)
            return c

        lax.fori_loop(0, num_block + 1, stage_of, 0)

        def update(moves):
            for i in range(half // 16):
                part = slice(16 * i, 16 * i + 16)
                w, u = wm[part, :], v[part, :]
                new = pm[part, :] + kick * (gm[part, :] - w / PRIOR_VAR)
                pm[part, :] = new
                total = jnp.broadcast_to(jnp.sum(g2[part, :], axis=1, keepdims=True), u.shape)
                new_q = q[part, :] + kick * (total - u / PRIOR_VAR)
                q[part, :] = new_q
                if moves:
                    w = w + step * new
                    wm[part, :] = w
                    wmb[part, :] = w.astype(BF16)
                    v[part, :] = u + step * new_q
                    gm[part, :] = jnp.zeros_like(w)
                    g2[part, :] = jnp.zeros_like(u)

        @pl.when(index < LEAPS)
        def _():
            update(True)

        @pl.when(index == LEAPS)
        def _():
            update(False)

        @pl.when(index == LEAPS - 1)
        def _():
            pack_small(small_w, wm, v, 0.0)
            end_begin(0)
        return carry

    lax.fori_loop(0, LEAPS + 1, gradient, 0)

    last = LEAPS % 2
    z = z_own[last] + z_peer[last]
    loss = jnp.maximum(z, 0.0) + jnp.log1p(jnp.exp(-jnp.abs(z))) - lab[...].astype(F32) * z

    def total(x):
        return jnp.sum(jnp.sum(x, axis=0, keepdims=True), axis=1, keepdims=True)

    squares = total(wm[...] * wm[...]) + total(v[...] * v[...]) / 128.0
    moving = total(pm[...] * pm[...]) + total(q[...] * q[...]) / 128.0
    energy = 0.5 * total(loss) + squares / (2.0 * PRIOR_VAR) + 0.5 * moving
    pack_small(small_p, pm, q, energy)
    end_begin(1)
    end_relay(0)
    end_relay(1)
    end_finish(0)
    end_finish(1)
    for ticket in range(14):
        x_sent(ticket)


def run_kernel(step, xs, lab, w1, w2, p1, p2, devices):
    num_feat, chains, hidden = w1.shape
    num_rows = xs.shape[1] * devices
    half = hidden // 2
    vmem = pl.BlockSpec(memory_space=pltpu.VMEM)
    hbm = pl.BlockSpec(memory_space=pl.ANY)
    big = jax.ShapeDtypeStruct((devices, half, MAIN), F32)
    small = jax.ShapeDtypeStruct((devices, SMALL, half), F32)
    blocks = num_rows // BLOCK
    dma = pltpu.SemaphoreType.DMA
    return pl.pallas_call(
        functools.partial(chain_kernel, step),
        out_shape=[big, small, big, small],
        in_specs=[hbm, hbm, hbm, vmem, hbm, vmem],
        out_specs=[hbm] * 4,
        scratch_shapes=[
            pltpu.VMEM((num_feat, num_rows), BF16),
            pltpu.VMEM((1, num_rows), jnp.int32),
            pltpu.VMEM((num_feat, chains, hidden), F32),
            pltpu.VMEM((hidden, num_feat), F32),
            pltpu.VMEM((half, num_rows), F32),
            pltpu.VMEM((half, BLOCK), BF16),
            pltpu.VMEM((half, num_feat), F32),
            pltpu.VMEM((half, 128), F32),
            pltpu.VMEM((half, num_feat), F32),
            pltpu.VMEM((half, 128), F32),
            pltpu.VMEM((half, num_feat), F32),
            pltpu.VMEM((half, 128), F32),
            pltpu.VMEM((half, num_feat), BF16),
            pltpu.VMEM((2, 1, num_rows), F32),
            pltpu.VMEM((2, 1, num_rows), F32),
            pltpu.VMEM((SMALL, half), F32),
            pltpu.VMEM((SMALL, half), F32),
            dma((4,)),
            dma((2, 14)),
            dma((2, 16)),
            dma((2, blocks)),
            dma((2, blocks)),
            dma((2, 3, 7)),
            dma((2, 3, devices)),
            dma((2, 3)),
        ],
        compiler_params=pltpu.CompilerParams(
            collective_id=0, has_side_effects=True, vmem_limit_bytes=62 * 2 ** 20),
    )(xs, lab, w1, w2, p1, p2)


def place_kernel(gw, gws, gp, gps, end_w, end_w2, end_p, end_p2, energy):
    step = pl.program_id(0)
    tiles = MAIN // 128
    chains = end_w.shape[1]
    rest = gws.shape[1] - 8

    @pl.when(step < tiles)
    def _():
        for g, end in ((gw, end_w), (gp, end_p)):
            for c in range(chains):
                end[:, c, :] = jnp.concatenate([g[2 * c], g[2 * c + 1]], axis=0).T

    @pl.when(step == tiles)
    def _():
        for g, end, end2 in ((gws, end_w, end_w2), (gps, end_p, end_p2)):
            for c in range(chains):
                both = jnp.concatenate([g[2 * c], g[2 * c + 1]], axis=1)
                end[0:rest, c, :] = both[0:rest, :]
                end2[c:c + 1, :] = both[rest:rest + 1, :]
        for c in range(chains):
            row = slice(rest + 1, rest + 2)
            sums = gps[2 * c, row, 0:128] + gps[2 * c + 1, row, 0:128]
            energy[c:c + 1, :] = sums


def place(gw, gws, gp, gps, num_feat, chains, hidden):
    tiles = MAIN // 128
    devices, half = gw.shape[0], gw.shape[1]
    big = pl.BlockSpec((devices, half, 128), lambda i: (0, 0, jnp.minimum(i, tiles - 1)))
    small = pl.BlockSpec(gws.shape, lambda i: (0, 0, 0))
    out = pl.BlockSpec((128, chains, hidden), lambda i: (i, 0, 0))
    shape = jax.ShapeDtypeStruct((num_feat, chains, hidden), F32)
    row = jax.ShapeDtypeStruct((chains, hidden), F32)
    flat = pl.BlockSpec((chains, hidden), lambda i: (0, 0))
    return pl.pallas_call(
        place_kernel, grid=(tiles + 1,),
        out_shape=[shape, row, shape, row, jax.ShapeDtypeStruct((chains, 128), F32)],
        in_specs=[big, small, big, small],
        out_specs=[out, flat, out, flat, pl.BlockSpec((chains, 128), lambda i: (0, 0))],
        compiler_params=pltpu.CompilerParams(vmem_limit_bytes=62 * 2 ** 20),
    )(gw, gws, gp, gps)


def solution(mesh):
    row_spec = P('data', None)
    label_spec = P('data')
    in_spec = P(None, 'parts', None)
    out_spec = P('parts', None)
    chain_spec = P('parts')
    devices = mesh.shape['data']

    def run_chains(feats, labels, w_in, w_out, mom_in, mom_out):
        num_rows, num_feat = feats.shape
        chains, hidden = w_out.shape
        step = 1.0 / math.sqrt(num_rows * (num_feat + hidden))

        def device_body(x_rows, y_rows, w1, w2, p1, p2):
            gw, gws, gp, gps = run_kernel(step, x_rows.T, y_rows[None, :], w1, w2, p1, p2, devices)
            *state, energy = place(gw, gws, gp, gps, num_feat, chains, hidden)
            return *state, energy[:, 0]

        mapped = jax.shard_map(device_body, mesh=mesh, in_specs=(row_spec, label_spec, in_spec, out_spec, in_spec, out_spec), out_specs=(in_spec, out_spec, in_spec, out_spec, chain_spec), check_vma=False)
        return mapped(feats, labels, w_in, w_out, mom_in, mom_out)

    return run_chains
```

```python
import functools
import math
import jax
import jax.numpy as jnp
from jax import lax
from jax.experimental import pallas as pl
from jax.experimental.pallas import tpu as pltpu
from jax.sharding import PartitionSpec as P

LEAPS = 16
PRIOR_VAR = 1.0
MAIN = 768
BLOCK = 4096
CHUNK = 256
DEPTH = 512
PIECE = 512
SMALL = 24
MESH = pl.DeviceIdType.MESH
F32 = jnp.float32
BF16 = jnp.bfloat16
NT = (((1,), (1,)), ((), ()))


def chain_kernel(step, x_hbm, lab_ref, w1_hbm, w2_ref, p1_hbm, p2_ref,
                 end_w, end_ws, end_p, end_ps,
                 xt, lab, stage, turn, act, bt, gm, g2, wm, v, pm, q, wmb,
                 z_own, z_peer, small_w, small_p,
                 load_sem, x_send, x_recv, send_sem, recv_sem, end_send, end_recv, end_load):
    num_feat, num_rows = xt.shape
    num_block = num_rows // BLOCK
    half = wm.shape[0]
    rest = num_feat - MAIN
    me = lax.axis_index("data")
    chip = me // 2
    core = lax.rem(me, 2)
    x_bit = lax.rem(chip, 2)
    y_bit = chip // 2
    peer = me + 1 - 2 * core
    x_near = me + 2 - 4 * x_bit
    y_near = me + 4 - 8 * y_bit
    far = x_near + 4 - 8 * y_bit

    barrier = pltpu.get_barrier_semaphore()
    for other in (peer, x_near, y_near):
        pl.semaphore_signal(barrier, inc=1, device_id={"data": other}, device_id_type=MESH)

    def rows_of(position, size):
        return pl.ds(pl.multiple_of(position * size, size), size)

    own = [2 * core, 2 * core + 1]
    mine = rows_of(core, 2 * PIECE)
    loads = [
        pltpu.make_async_copy(x_hbm, xt.at[:, mine], load_sem.at[0]),
        pltpu.make_async_copy(lab_ref, lab.at[:, mine], load_sem.at[1]),
    ]
    for c in loads:
        c.start()
    load_w = pltpu.make_async_copy(w1_hbm, stage, load_sem.at[2])
    load_p = pltpu.make_async_copy(p1_hbm, stage, load_sem.at[3])
    load_w.start()
    pl.semaphore_wait(barrier, 3)
    for c in loads:
        c.wait()

    def x_copies(src, dst, device, ticket):
        a, b = rows_of(src, PIECE), rows_of(dst, PIECE)
        pairs = ((xt.at[:, a], xt.at[:, b]), (lab.at[:, a], lab.at[:, b]))
        return [pltpu.make_async_remote_copy(
            src_ref=s, dst_ref=d, send_sem=x_send.at[i, ticket], recv_sem=x_recv.at[i, dst],
            device_id={"data": device}, device_id_type=MESH) for i, (s, d) in enumerate(pairs)]

    def x_go(src, dst, device, ticket):
        for c in x_copies(src, dst, device, ticket):
            c.start()

    def x_arrived(position):
        for c in x_copies(position, position, peer, 0):
            c.wait_recv()

    def x_sent(ticket):
        for c in x_copies(0, 0, peer, ticket):
            c.wait_send()

    def near_pos(h, which, owner):
        return 4 + 4 * h + 2 * which + owner

    def far_pos(h, owner):
        return 12 + 2 * h + owner

    for h in range(2):
        x_go(own[h], near_pos(h, 0, core), x_near, 3 * h)
        x_go(own[h], near_pos(h, 1, core), y_near, 3 * h + 1)
        x_go(own[h], own[h], peer, 3 * h + 2)

    def part_of(out):
        for d in range(MAIN // 128):
            turn[:, d * 128:(d + 1) * 128] = stage[d * 128:(d + 1) * 128, chip, :].T
        tail = stage[MAIN:MAIN + rest, chip, :]
        tail = jnp.concatenate([tail, jnp.zeros((128 - rest, tail.shape[1]), F32)], axis=0)
        turn[:, MAIN:MAIN + rest] = tail.T[:, 0:rest]
        out[...] = turn[pl.ds(pl.multiple_of(core * half, 8), half), :]

    def row_of(u, out):
        turn[:, 0:128] = jnp.broadcast_to(u[pl.ds(chip, 1), :], (128, u.shape[1])).T
        out[...] = turn[pl.ds(pl.multiple_of(core * half, 8), half), 0:128]

    load_w.wait()
    part_of(wm)
    load_p.start()
    row_of(w2_ref, v)
    wmb[...] = wm[...].astype(BF16)
    row_of(p2_ref, q)
    gm[...] = jnp.zeros_like(gm)
    g2[...] = jnp.zeros_like(g2)

    other = 1 - core
    x_arrived(2 * other)
    x_arrived(2 * other + 1)

    def arrivals(k):
        if k == 1:
            for which in range(2):
                x_arrived(near_pos(0, which, core))
                if which == 0:
                    x_go(near_pos(0, 0, core), far_pos(0, core), y_near, 6)
                x_go(near_pos(0, which, core), near_pos(0, which, core), peer, 7 + which)
            for which in range(2):
                x_arrived(near_pos(0, which, other))
        elif k == 2:
            for which in (1, 0):
                x_arrived(near_pos(1, which, core))
                if which == 1:
                    x_go(near_pos(1, 1, core), far_pos(1, core), x_near, 9)
                x_go(near_pos(1, which, core), near_pos(1, which, core), peer, 10 + which)
            for which in range(2):
                x_arrived(near_pos(1, which, other))
        elif k == 3:
            for h in range(2):
                x_arrived(far_pos(h, core))
                x_go(far_pos(h, core), far_pos(h, core), peer, 12 + h)
            for h in range(2):
                x_arrived(far_pos(h, other))

    def z_copy(slot, block):
        span = rows_of(block, BLOCK)
        return pltpu.make_async_remote_copy(
            src_ref=z_own.at[slot, :, span], dst_ref=z_peer.at[slot, :, span],
            send_sem=send_sem.at[slot, block], recv_sem=recv_sem.at[slot, block],
            device_id={"data": peer}, device_id_type=MESH)

    def forward(block, slot):
        base = block * BLOCK
        for n in range(BLOCK // CHUNK):
            rows = pl.ds(pl.multiple_of(base + n * CHUNK, CHUNK), CHUNK)
            pre = jnp.dot(wmb[:, 0:MAIN], xt[0:MAIN, rows], preferred_element_type=F32)
            pre = pre + jnp.dot(wmb[:, MAIN:], xt[MAIN:, rows], preferred_element_type=F32)
            for j in range(CHUNK // 128):
                cols = pl.ds(pl.multiple_of(base + n * CHUNK + j * 128, 128), 128)
                t = jnp.tanh(pre[:, j * 128:(j + 1) * 128])
                act[:, cols] = t
                z_own[slot, :, cols] = jnp.sum(t * v[...], axis=0, keepdims=True)
        z_copy(slot, block).start()

    def backward(block, slot):
        z_copy(slot, block).wait()
        base = block * BLOCK
        for n in range(BLOCK // DEPTH):
            for j in range(DEPTH // 128):
                cols = pl.ds(pl.multiple_of(base + n * DEPTH + j * 128, 128), 128)
                z = z_own[slot, :, cols] + z_peer[slot, :, cols]
                r = lab[:, cols].astype(F32) - jax.nn.sigmoid(z)
                t = act[:, cols]
                rb = jnp.broadcast_to(r, t.shape)
                bt[:, pl.ds(n * DEPTH + j * 128, 128)] = ((rb * v[...]) * (1.0 - t * t)).astype(BF16)
                g2[...] += rb * t
            rows = pl.ds(pl.multiple_of(base + n * DEPTH, DEPTH), DEPTH)
            b = bt[:, n * DEPTH:(n + 1) * DEPTH]
            gm[...] += lax.dot_general(b, xt[:, rows], NT, preferred_element_type=F32)

    big = (wm, pm)
    small = (small_w, small_p)
    out_big = (end_w, end_p)
    out_small = (end_ws, end_ps)
    part = half // 2

    def end_pair(t, piece, source):
        if piece == 2:
            return small[t], out_small[t].at[source]
        span = pl.ds(piece * part, part)
        return big[t].at[span, pl.ds(0, MAIN)], out_big[t].at[source, span, :]

    def end_copy(t, piece, source, device, ticket, first):
        src, dst = end_pair(t, piece, source)
        return pltpu.make_async_remote_copy(
            src_ref=src if first else dst, dst_ref=dst,
            send_sem=end_send.at[t, piece, ticket], recv_sem=end_recv.at[t, piece, source],
            device_id={"data": device}, device_id_type=MESH)

    def end_arrived(t, piece, source):
        end_copy(t, piece, source, peer, 0, False).wait_recv()

    def end_begin(t):
        for piece in (0, 2, 1):
            end_copy(t, piece, me, x_near, 0, True).start()
            end_copy(t, piece, me, y_near, 1, True).start()
        for piece in (0, 1, 2):
            end_copy(t, piece, me, peer, 2, True).start()
            src, dst = end_pair(t, piece, me)
            pltpu.make_async_copy(src, dst, end_load.at[t, piece]).start()

    def end_relay(t):
        for piece in (0, 2, 1):
            end_arrived(t, piece, x_near)
            if piece != 1:
                end_copy(t, piece, x_near, y_near, 3, False).start()
            end_arrived(t, piece, y_near)
            if piece == 1:
                end_copy(t, piece, y_near, x_near, 3, False).start()
            end_copy(t, piece, x_near, peer, 4, False).start()
            end_copy(t, piece, y_near, peer, 5, False).start()

    def end_finish(t):
        for piece in (0, 2, 1):
            end_arrived(t, piece, far)
            end_copy(t, piece, far, peer, 6, False).start()
        for piece in (0, 1, 2):
            for delta in (me, x_near, y_near, far):
                end_arrived(t, piece, delta + 1 - 2 * core)
            for ticket in range(7):
                end_copy(t, piece, me, peer, ticket, False).wait_send()
            src, dst = end_pair(t, piece, me)
            pltpu.make_async_copy(src, dst, end_load.at[t, piece]).wait()

    def pack_small(buf, m, u, extra):
        wide = jnp.concatenate([m[:, MAIN:MAIN + rest], u[:, 0:8], jnp.zeros((half, 104), F32)], axis=1)
        flat = wide.T
        buf[0:rest, :] = flat[0:rest, :]
        buf[rest:SMALL, :] = jnp.where(lax.broadcasted_iota(jnp.int32, (SMALL - rest, half), 0) == 0, flat[rest:SMALL, :], extra)

    def gradient(index, carry):
        slot = lax.rem(index, 2)
        edge = jnp.logical_or(index == 0, index == LEAPS)
        kick = jnp.where(edge, 0.5 * step, step).astype(F32)
        def stage_of(k, c):
            for j in range(1, 4):
                @pl.when(jnp.logical_and(index == 0, k == j * 4 * PIECE // BLOCK))
                def _():
                    arrivals(j)
                    if j == 1:
                        load_p.wait()
                        part_of(pm)

            @pl.when(k < num_block)
            def _():
                forward(k, slot)

            @pl.when(k > 0)
            def _():
                backward(k - 1, slot)
            return c

        lax.fori_loop(0, num_block + 1, stage_of, 0)

        def update(moves):
            for i in range(half // 16):
                part = slice(16 * i, 16 * i + 16)
                w, u = wm[part, :], v[part, :]
                new = pm[part, :] + kick * (gm[part, :] - w / PRIOR_VAR)
                pm[part, :] = new
                total = jnp.broadcast_to(jnp.sum(g2[part, :], axis=1, keepdims=True), u.shape)
                new_q = q[part, :] + kick * (total - u / PRIOR_VAR)
                q[part, :] = new_q
                if moves:
                    w = w + step * new
                    wm[part, :] = w
                    wmb[part, :] = w.astype(BF16)
                    v[part, :] = u + step * new_q
                    gm[part, :] = jnp.zeros_like(w)
                    g2[part, :] = jnp.zeros_like(u)

        @pl.when(index < LEAPS)
        def _():
            update(True)

        @pl.when(index == LEAPS)
        def _():
            update(False)

        @pl.when(index == LEAPS - 1)
        def _():
            pack_small(small_w, wm, v, 0.0)
            end_begin(0)
        return carry

    lax.fori_loop(0, LEAPS + 1, gradient, 0)

    last = LEAPS % 2
    z = z_own[last] + z_peer[last]
    loss = jnp.maximum(z, 0.0) + jnp.log1p(jnp.exp(-jnp.abs(z))) - lab[...].astype(F32) * z

    def total(x):
        return jnp.sum(jnp.sum(x, axis=0, keepdims=True), axis=1, keepdims=True)

    squares = total(wm[...] * wm[...]) + total(v[...] * v[...]) / 128.0
    moving = total(pm[...] * pm[...]) + total(q[...] * q[...]) / 128.0
    energy = 0.5 * total(loss) + squares / (2.0 * PRIOR_VAR) + 0.5 * moving
    pack_small(small_p, pm, q, energy)
    end_begin(1)
    end_relay(0)
    end_relay(1)
    end_finish(0)
    end_finish(1)
    for ticket in range(14):
        x_sent(ticket)


def run_kernel(step, xs, lab, w1, w2, p1, p2, devices):
    num_feat, chains, hidden = w1.shape
    num_rows = xs.shape[1] * devices
    half = hidden // 2
    vmem = pl.BlockSpec(memory_space=pltpu.VMEM)
    hbm = pl.BlockSpec(memory_space=pl.ANY)
    big = jax.ShapeDtypeStruct((devices, half, MAIN), F32)
    small = jax.ShapeDtypeStruct((devices, SMALL, half), F32)
    blocks = num_rows // BLOCK
    dma = pltpu.SemaphoreType.DMA
    return pl.pallas_call(
        functools.partial(chain_kernel, step),
        out_shape=[big, small, big, small],
        in_specs=[hbm, hbm, hbm, vmem, hbm, vmem],
        out_specs=[hbm] * 4,
        scratch_shapes=[
            pltpu.VMEM((num_feat, num_rows), BF16),
            pltpu.VMEM((1, num_rows), jnp.int32),
            pltpu.VMEM((num_feat, chains, hidden), F32),
            pltpu.VMEM((hidden, num_feat), F32),
            pltpu.VMEM((half, num_rows), F32),
            pltpu.VMEM((half, BLOCK), BF16),
            pltpu.VMEM((half, num_feat), F32),
            pltpu.VMEM((half, 128), F32),
            pltpu.VMEM((half, num_feat), F32),
            pltpu.VMEM((half, 128), F32),
            pltpu.VMEM((half, num_feat), F32),
            pltpu.VMEM((half, 128), F32),
            pltpu.VMEM((half, num_feat), BF16),
            pltpu.VMEM((2, 1, num_rows), F32),
            pltpu.VMEM((2, 1, num_rows), F32),
            pltpu.VMEM((SMALL, half), F32),
            pltpu.VMEM((SMALL, half), F32),
            dma((4,)),
            dma((2, 14)),
            dma((2, 16)),
            dma((2, blocks)),
            dma((2, blocks)),
            dma((2, 3, 7)),
            dma((2, 3, devices)),
            dma((2, 3)),
        ],
        compiler_params=pltpu.CompilerParams(
            collective_id=0, has_side_effects=True, vmem_limit_bytes=62 * 2 ** 20),
    )(xs, lab, w1, w2, p1, p2)


def place_kernel(gw, gws, gp, gps, end_w, end_w2, end_p, end_p2, energy):
    step = pl.program_id(0)
    tiles = MAIN // 128
    chains = end_w.shape[1]
    rest = gws.shape[1] - 8

    @pl.when(step < tiles)
    def _():
        for g, end in ((gw, end_w), (gp, end_p)):
            for c in range(chains):
                end[:, c, :] = jnp.concatenate([g[2 * c], g[2 * c + 1]], axis=0).T

    @pl.when(step == tiles)
    def _():
        for g, end, end2 in ((gws, end_w, end_w2), (gps, end_p, end_p2)):
            for c in range(chains):
                both = jnp.concatenate([g[2 * c], g[2 * c + 1]], axis=1)
                end[0:rest, c, :] = both[0:rest, :]
                end2[c:c + 1, :] = both[rest:rest + 1, :]
        for c in range(chains):
            row = slice(rest + 1, rest + 2)
            sums = gps[2 * c, row, 0:128] + gps[2 * c + 1, row, 0:128]
            energy[c:c + 1, :] = sums


def place(gw, gws, gp, gps, num_feat, chains, hidden):
    tiles = MAIN // 128
    devices, half = gw.shape[0], gw.shape[1]
    big = pl.BlockSpec((devices, half, 128), lambda i: (0, 0, jnp.minimum(i, tiles - 1)))
    small = pl.BlockSpec(gws.shape, lambda i: (0, 0, 0))
    out = pl.BlockSpec((128, chains, hidden), lambda i: (i, 0, 0))
    shape = jax.ShapeDtypeStruct((num_feat, chains, hidden), F32)
    row = jax.ShapeDtypeStruct((chains, hidden), F32)
    flat = pl.BlockSpec((chains, hidden), lambda i: (0, 0))
    return pl.pallas_call(
        place_kernel, grid=(tiles + 1,),
        out_shape=[shape, row, shape, row, jax.ShapeDtypeStruct((chains, 128), F32)],
        in_specs=[big, small, big, small],
        out_specs=[out, flat, out, flat, pl.BlockSpec((chains, 128), lambda i: (0, 0))],
        compiler_params=pltpu.CompilerParams(vmem_limit_bytes=62 * 2 ** 20),
    )(gw, gws, gp, gps)


def solution(mesh):
    row_spec = P('data', None)
    label_spec = P('data')
    in_spec = P(None, 'parts', None)
    out_spec = P('parts', None)
    chain_spec = P('parts')
    devices = mesh.shape['data']

    def run_chains(feats, labels, w_in, w_out, mom_in, mom_out):
        num_rows, num_feat = feats.shape
        chains, hidden = w_out.shape
        step = 1.0 / math.sqrt(num_rows * (num_feat + hidden))

        def device_body(x_rows, y_rows, w1, w2, p1, p2):
            gw, gws, gp, gps = run_kernel(step, x_rows.T, y_rows[None, :], w1, w2, p1, p2, devices)
            *state, energy = place(gw, gws, gp, gps, num_feat, chains, hidden)
            return *state, energy[:, 0]

        mapped = jax.shard_map(device_body, mesh=mesh, in_specs=(row_spec, label_spec, in_spec, out_spec, in_spec, out_spec), out_specs=(in_spec, out_spec, in_spec, out_spec, chain_spec), check_vma=False)
        return mapped(feats, labels, w_in, w_out, mom_in, mom_out)

    return run_chains
```
